32 devices in a mesh: seq: 8 (over y, x, core), rep: 4 (over z).
Axes of the slice: x: 2, y: 2, z: 4, core: 2. Of those that a mesh axis runs over, the one named last changes fastest.
Arguments:
- prefix_cache: bfloat16 [2, 2, 1024, 4096], P(None, None, 'seq', 'rep'), may hold values from -5 to 5
- queries: bfloat16 [2, 32, 4096], P(None, ('seq', 'rep')), may hold values from -12 to 12
- suffix_cache: bfloat16 [2, 32, 2, 128, 1024], P(None, ('seq', 'rep')), may hold values from -9 to 9
- suffix_lengths: int32 [32], replicated, may hold values from 1 to 128, as said below
- slot_request: int32 [32], P(('seq', 'rep')), may hold values from 0 to 31, each once
Outputs:
- attended: bfloat16 [2, 32, 4096], P(None, ('seq', 'rep'))
The draws below stay inside these ranges and needn't reach their ends.
Inputs may be any that keep to these rules, and one draw needn't show every extreme that they name: `suffix_lengths`: every request has 1 to 128 suffix tokens; some request has exactly 128. `slot_request`: every request id stands in exactly one slot.
All inputs are finite; a program needn't handle non-finite values.
Results may differ from the reference program's by a relative error of at most 0.005.
Values may be sent and summed in bfloat16 or wider, within the bound.
A program may use at most 64 MiB of HBM per device.

```python
import jax
import jax.numpy as jnp
from jax import lax

QH = 32
KVH = 8
HD = 128
LAYERS = 2
SUF = 128
GROUP = 4
KV_FEAT = 1024
PREFIX = 4096
REQUESTS = 32


def draw_prefix_cache(key, part):
    fresh_key = jax.random.fold_in(key, 11)
    shape_full = (LAYERS, 2, KVH * HD, PREFIX)
    drawn = jnp.clip(jax.random.normal(fresh_key, shape_full, jnp.float32), -5.0, 5.0)
    return drawn.astype(jnp.bfloat16)


def draw_queries(key, part):
    fresh_key = jax.random.fold_in(key, 13)
    shape_full = (LAYERS, REQUESTS, QH * HD)
    drawn = jnp.clip(3.0 * jax.random.normal(fresh_key, shape_full, jnp.float32), -12.0, 12.0)
    return drawn.astype(jnp.bfloat16)


def draw_suffix_lengths(key, part):
    length_key, top_key = jax.random.split(jax.random.fold_in(key, 23))
    drawn = jax.random.randint(length_key, (REQUESTS,), 1, SUF + 1)
    top_index = jax.random.randint(top_key, (), 0, REQUESTS)
    return jnp.where(jnp.arange(REQUESTS) == top_index, SUF, drawn).astype(jnp.int32)


def level_of(stream_key, extent, cuts, smallest, high):
    def one(position, shards_of):
        steps = jax.random.uniform(jax.random.fold_in(jax.random.fold_in(stream_key, 6), position), (shards_of,), jnp.float32, smallest / len(cuts), high / len(cuts))
        return jnp.repeat(jnp.exp(steps), extent[position] // shards_of).reshape((-1,) + (1,) * (len(extent) - position - 1))

    factor_of = one(*cuts[0])
    for cut in cuts[1:]:
        factor_of = factor_of * one(*cut)
    return factor_of


def gaussian(stream_key, extent, scale, limit, cuts=(), held_as=jnp.bfloat16):
    array = scale * jax.random.normal(stream_key, extent, jnp.float32)
    if cuts:
        array = array * level_of(stream_key, extent, cuts, -0.22, 0.18)
    return jnp.clip(array, -limit, limit).astype(held_as)


def setup_inputs(seed: int = 0) -> dict:
    keys = jax.random.split(jax.random.key(seed), 6)
    return {
        "prefix_cache": draw_prefix_cache(jax.random.fold_in(keys[5], 71), 0),
        "queries": draw_queries(jax.random.fold_in(keys[5], 71), 0),
        "suffix_cache": gaussian(keys[2], (LAYERS, REQUESTS, 2, SUF, KV_FEAT), 1.5, 9.0, ((1, 32),)),
        "suffix_lengths": draw_suffix_lengths(jax.random.fold_in(keys[5], 71), 0),
        "slot_request": jax.random.permutation(keys[4], REQUESTS).astype(jnp.int32),
    }


neg_fill = -1.0e30
block_rows = 8


def attend(query_rows, key_block, value_block, suffix_rows, length_rows):
    row_count = query_rows.shape[0]
    score_scale = HD ** -0.5
    shaped = query_rows.astype(jnp.float32).reshape(row_count, KVH, GROUP, HD)
    scores = jnp.einsum("rhgd,hdp->rhgp", shaped, key_block, precision=lax.Precision.HIGHEST) * score_scale
    prefix_top = jnp.max(scores, axis=3)
    weights = jnp.exp(scores - prefix_top[..., None]).astype(jnp.bfloat16)
    weights = lax.optimization_barrier(weights).astype(jnp.float32)
    prefix_den = jnp.sum(weights, axis=3)
    prefix_num = jnp.einsum("rhgp,hdp->rhgd", weights, value_block, precision=lax.Precision.HIGHEST)
    suffix_keys = suffix_rows[:, 0].astype(jnp.float32).reshape(row_count, SUF, KVH, HD)
    suffix_values = suffix_rows[:, 1].astype(jnp.float32).reshape(row_count, SUF, KVH, HD)
    suffix_scores = jnp.einsum("rhgd,rshd->rhgs", shaped, suffix_keys, precision=lax.Precision.HIGHEST) * score_scale
    valid_mask = (jnp.arange(SUF, dtype=jnp.int32)[None, :] < length_rows[:, None])[:, None, None, :]
    suffix_scores = jnp.where(valid_mask, suffix_scores, neg_fill)
    suffix_top = jnp.max(suffix_scores, axis=3)
    suffix_weights = jnp.where(valid_mask, jnp.exp(suffix_scores - suffix_top[..., None]), 0.0).astype(jnp.bfloat16)
    suffix_weights = lax.optimization_barrier(suffix_weights).astype(jnp.float32)
    suffix_den = jnp.sum(suffix_weights, axis=3)
    suffix_num = jnp.einsum("rhgs,rshd->rhgd", suffix_weights, suffix_values, precision=lax.Precision.HIGHEST)
    both_top = jnp.maximum(prefix_top, suffix_top)
    prefix_scale = jnp.exp(prefix_top - both_top)
    suffix_scale = jnp.exp(suffix_top - both_top)
    total_den = prefix_scale * prefix_den + suffix_scale * suffix_den
    mixed = (prefix_scale[..., None] * prefix_num + suffix_scale[..., None] * suffix_num) / total_den[..., None]
    return mixed.reshape(row_count, QH * HD).astype(jnp.bfloat16)


def reference(prefix_cache, queries, suffix_cache, suffix_lengths, slot_request):
    lengths = suffix_lengths[slot_request]
    blocks = REQUESTS // block_rows
    results = []
    for layer_index in range(LAYERS):
        key_block = prefix_cache[layer_index, 0].astype(jnp.float32).reshape(KVH, HD, PREFIX)
        value_block = prefix_cache[layer_index, 1].astype(jnp.float32).reshape(KVH, HD, PREFIX)
        query_rows = queries[layer_index].reshape(blocks, block_rows, QH * HD)
        suffix_rows = suffix_cache[layer_index].reshape(blocks, block_rows, 2, SUF, KVH * HD)
        length_rows = lengths.reshape(blocks, block_rows)

        def one_block(packed):
            return attend(packed[0], key_block, value_block, packed[1], packed[2])

        attended = lax.map(one_block, (query_rows, suffix_rows, length_rows))
        results.append(attended.reshape(REQUESTS, QH * HD))
    return jnp.stack(results)
```

```python
import functools

import jax
import jax.numpy as jnp
from jax import lax
from jax.experimental import pallas as pl
from jax.experimental.pallas import tpu as pltpu
from jax.sharding import PartitionSpec as P

QH = 32
KVH = 8
HD = 128
GROUP = QH // KVH
neg_fill = -1e30
LOG2E = 1.4426950408889634
SCALE = HD ** -0.5 * LOG2E
CHUNK = 32
NT = (((1,), (1,)), ((), ()))


def layer_rows(shape, layers):
    return (lax.broadcasted_iota(jnp.int32, shape, 0) // GROUP) % layers


def kernel(
    n_rep, n_all, span, layers,
    lengths_ref, slot_ref, cache_ref, q_ref, suffix_ref, out_ref,
    kv, sfx, q_row, q_f32, q_send, q_recv, o_send, o_recv,
    load_sem, q_send_sem, q_recv_sem, o_send_sem, o_recv_sem,
):
    rows = layers * GROUP
    me_seq = lax.axis_index("seq")
    me_rep = lax.axis_index("rep")
    me = me_seq * n_rep + me_rep

    def place(k):
        other = lax.rem(me + k, n_all)
        return other, {"seq": other // n_rep, "rep": lax.rem(other, n_rep)}

    load_q = pltpu.make_async_copy(q_ref, q_row, load_sem.at[0])
    load_q.start()
    load_sfx = pltpu.make_async_copy(suffix_ref, sfx, load_sem.at[1])
    load_sfx.start()
    load_kv = pltpu.make_async_copy(cache_ref, kv, load_sem.at[2])
    load_kv.start()

    barrier = pltpu.get_barrier_semaphore()

    @pl.loop(1, n_all)
    def _(k):
        _, where = place(k)
        pl.semaphore_signal(barrier, inc=1, device_id=where, device_id_type=pl.DeviceIdType.MESH)

    load_q.wait()
    for l in range(layers):
        for k in range(QH):
            h, g = k // GROUP, k % GROUP
            q_f32[h, l * GROUP + g : l * GROUP + g + 1, :] = q_row[
                l, :, k * HD : (k + 1) * HD
            ].astype(jnp.float32)
    q_send[...] = q_f32[...].astype(jnp.bfloat16)

    pl.semaphore_wait(barrier, n_all - 1)

    my_head = me_seq // span
    own_q = pltpu.make_async_copy(q_send.at[my_head], q_recv.at[me], q_recv_sem)
    own_q.start()

    @pl.loop(1, n_all)
    def _(k):
        other, where = place(k)
        pltpu.make_async_remote_copy(
            src_ref=q_send.at[other // n_rep // span],
            dst_ref=q_recv.at[me],
            send_sem=q_send_sem,
            recv_sem=q_recv_sem,
            device_id=where,
            device_id_type=pl.DeviceIdType.MESH,
        ).start()

    load_sfx.wait()
    s_rows = KVH * rows
    length = lengths_ref[slot_ref[0]]
    q_all = q_f32[...].reshape(s_rows, HD)
    head_of = lax.broadcasted_iota(jnp.int32, (s_rows, HD), 0) // rows
    q_diag = jnp.concatenate(
        [jnp.where(head_of == h, q_all, 0.0) for h in range(KVH)], axis=1
    ).astype(jnp.bfloat16)
    suf = sfx.shape[3]
    lay_s = layer_rows((s_rows, suf), layers)
    scores = jnp.zeros((s_rows, suf), jnp.float32)
    for l in range(layers):
        part = lax.dot_general(q_diag, sfx[l, 0, 0], NT, preferred_element_type=jnp.float32)
        scores = jnp.where(lay_s == l, part, scores)
    valid = lax.broadcasted_iota(jnp.int32, (s_rows, suf), 1) < length
    scores = jnp.where(valid, scores * SCALE, neg_fill)
    s_top = jnp.max(scores, axis=1, keepdims=True)
    s_w = jnp.where(valid, jnp.exp2(scores - s_top), 0.0).astype(jnp.bfloat16)
    s_den = jnp.sum(s_w.astype(jnp.float32), axis=1, keepdims=True)
    lay_h = layer_rows((s_rows, HD), layers)
    s_num = jnp.zeros((s_rows, HD), jnp.float32)
    for l in range(layers):
        part = jnp.dot(s_w, sfx[l, 0, 1], preferred_element_type=jnp.float32)
        for h in range(KVH):
            s_num = jnp.where(
                (head_of == h) & (lay_h == l), part[:, h * HD : (h + 1) * HD], s_num
            )

    load_kv.wait()
    pltpu.make_async_copy(q_recv, q_recv, q_recv_sem).wait()

    chunk = min(CHUNK, n_all)
    c_rows = chunk * rows
    positions = kv.shape[3]

    def one_chunk(base):
        q_c = q_recv[pl.ds(base, chunk)].astype(jnp.float32).reshape(c_rows, HD)
        lay = layer_rows((c_rows, HD), layers)
        q_c = jnp.concatenate(
            [jnp.where(lay == l, q_c, 0.0) for l in range(layers)], axis=1
        ).astype(jnp.bfloat16)
        keys = kv[:, 0].reshape(layers * HD, positions)
        values = kv[:, 1].reshape(layers * HD, positions)
        s = jnp.dot(q_c, keys, preferred_element_type=jnp.float32) * SCALE
        top = jnp.max(s, axis=1, keepdims=True)
        w = jnp.exp2(s - top).astype(jnp.bfloat16)
        den = jnp.sum(w.astype(jnp.float32), axis=1, keepdims=True)
        num_all = lax.dot_general(w, values, NT, preferred_element_type=jnp.float32)
        num = num_all[:, :HD]
        for l in range(1, layers):
            num = jnp.where(lay == l, num_all[:, l * HD : (l + 1) * HD], num)
        lse = top + jnp.log2(den)
        high = lse.astype(jnp.bfloat16).astype(jnp.float32)
        mid = (lse - high).astype(jnp.bfloat16).astype(jnp.float32)
        low = lse - high - mid
        lane = lax.broadcasted_iota(jnp.int32, (c_rows, HD), 1)
        stat = jnp.where(lane == 0, high, jnp.where(lane == 1, mid, jnp.where(lane == 2, low, 0.0)))
        both = jnp.concatenate(
            [(num / den).reshape(chunk, rows, HD), stat.reshape(chunk, rows, HD)], axis=1
        )
        o_send[pl.ds(base, chunk)] = both.astype(jnp.bfloat16)

    if chunk == n_all:
        one_chunk(0)
    else:
        @pl.loop(0, n_all // chunk)
        def _(c):
            one_chunk(c * chunk)

    own_o = pltpu.make_async_copy(o_send.at[me], o_recv.at[me], o_recv_sem)
    own_o.start()

    @pl.loop(1, n_all)
    def _(k):
        other, where = place(k)
        pltpu.make_async_remote_copy(
            src_ref=o_send.at[other],
            dst_ref=o_recv.at[me],
            send_sem=o_send_sem,
            recv_sem=o_recv_sem,
            device_id=where,
            device_id_type=pl.DeviceIdType.MESH,
        ).start()

    s_out = (s_num / s_den).reshape(KVH, rows, HD)
    s_lse = (s_top + jnp.log2(s_den)).reshape(KVH, rows, 1)
    others = pl.ds(0, n_all - 1)
    sent_q = q_recv.at[others]
    pltpu.make_async_copy(sent_q, sent_q, q_send_sem).wait()
    pltpu.make_async_copy(o_recv, o_recv, o_recv_sem).wait()

    per_head = n_all // KVH
    for h in range(KVH):
        got = o_recv[h * per_head : (h + 1) * per_head].astype(jnp.float32)
        part = got[:, :rows]
        lse = jnp.sum(got[:, rows:], axis=2, keepdims=True)
        top = jnp.maximum(jnp.max(lse, axis=0), s_lse[h])
        wgt = jnp.exp2(lse - top[None])
        s_wgt = jnp.exp2(s_lse[h] - top)
        num = jnp.sum(wgt * part, axis=0) + s_wgt * s_out[h]
        den = jnp.sum(wgt, axis=0) + s_wgt
        mixed = num / den
        for l in range(layers):
            for g in range(GROUP):
                at = (h * GROUP + g) * HD
                r = l * GROUP + g
                out_ref[l, :, at : at + HD] = mixed[r : r + 1].astype(out_ref.dtype)

    sent_o = o_recv.at[others]
    pltpu.make_async_copy(sent_o, sent_o, o_send_sem).wait()


def attend(n_seq, n_rep, prefix_cache, queries, suffix_cache, suffix_lengths, slot_request):
    layers, _, width = queries.shape
    n_all = n_seq * n_rep
    features = prefix_cache.shape[2]
    span = HD // features
    if span > 1:
        groups = [[h * span + j for j in range(span)] for h in range(n_seq // span)]
        prefix_cache = lax.all_to_all(
            prefix_cache, "seq", split_axis=3, concat_axis=2, axis_index_groups=groups, tiled=True
        )
    rows = layers * GROUP
    any_spec = pl.BlockSpec(memory_space=pl.ANY)
    smem_spec = pl.BlockSpec(memory_space=pltpu.SMEM)
    return pl.pallas_call(
        functools.partial(kernel, n_rep, n_all, span, layers),
        out_shape=jax.ShapeDtypeStruct(queries.shape, queries.dtype),
        in_specs=[smem_spec, smem_spec, any_spec, any_spec, any_spec],
        out_specs=pl.BlockSpec(memory_space=pltpu.VMEM),
        scratch_shapes=[
            pltpu.VMEM(prefix_cache.shape, jnp.bfloat16),
            pltpu.VMEM(suffix_cache.shape, jnp.bfloat16),
            pltpu.VMEM(queries.shape, jnp.bfloat16),
            pltpu.VMEM((KVH, rows, HD), jnp.float32),
            pltpu.VMEM((KVH, rows, HD), jnp.bfloat16),
            pltpu.VMEM((n_all, rows, HD), jnp.bfloat16),
            pltpu.VMEM((n_all, 2 * rows, HD), jnp.bfloat16),
            pltpu.VMEM((n_all, 2 * rows, HD), jnp.bfloat16),
            pltpu.SemaphoreType.DMA((3,)),
            pltpu.SemaphoreType.DMA,
            pltpu.SemaphoreType.DMA,
            pltpu.SemaphoreType.DMA,
            pltpu.SemaphoreType.DMA,
        ],
        compiler_params=pltpu.CompilerParams(collective_id=0, has_side_effects=True),
    )(suffix_lengths, slot_request, prefix_cache, queries, suffix_cache)


def solution(mesh):
    in_specs = (
        P(None, None, "seq", "rep"),
        P(None, ("seq", "rep"), None),
        P(None, ("seq", "rep"), None, None, None),
        P(),
        P(("seq", "rep")),
    )
    return jax.shard_map(
        functools.partial(attend, mesh.shape["seq"], mesh.shape["rep"]),
        mesh=mesh,
        in_specs=in_specs,
        out_specs=P(None, ("seq", "rep"), None),
        check_vma=False,
    )
```

```python
import functools

import jax
import jax.numpy as jnp
from jax import lax
from jax.experimental import pallas as pl
from jax.experimental.pallas import tpu as pltpu
from jax.sharding import PartitionSpec as P

QH = 32
KVH = 8
HD = 128
GROUP = QH // KVH
neg_fill = -1e30
LOG2E = 1.4426950408889634
SCALE = HD ** -0.5 * LOG2E
CHUNK = 32
NT = (((1,), (1,)), ((), ()))


def layer_rows(shape, layers):
    return (lax.broadcasted_iota(jnp.int32, shape, 0) // GROUP) % layers


def kernel(
    n_rep, n_all, span, layers,
    lengths_ref, slot_ref, cache_ref, q_ref, suffix_ref, out_ref,
    kv, sfx, q_row, q_f32, q_send, q_recv, o_send, o_recv, lengths, slot,
    load_sem, q_send_sem, q_recv_sem, o_send_sem, o_recv_sem,
):
    rows = layers * GROUP
    me_seq = lax.axis_index("seq")
    me_rep = lax.axis_index("rep")
    me = me_seq * n_rep + me_rep

    def place(k):
        other = lax.rem(me + k, n_all)
        return other, {"seq": other // n_rep, "rep": lax.rem(other, n_rep)}

    load_q = pltpu.make_async_copy(q_ref, q_row, load_sem.at[0])
    load_q.start()
    load_len = pltpu.make_async_copy(lengths_ref, lengths, load_sem.at[3])
    load_len.start()
    load_slot = pltpu.make_async_copy(slot_ref, slot, load_sem.at[4])
    load_slot.start()
    load_sfx = pltpu.make_async_copy(suffix_ref, sfx, load_sem.at[1])
    load_sfx.start()
    load_kv = pltpu.make_async_copy(cache_ref, kv, load_sem.at[2])
    load_kv.start()

    barrier = pltpu.get_barrier_semaphore()

    @pl.loop(1, n_all)
    def _(k):
        _, where = place(k)
        pl.semaphore_signal(barrier, inc=1, device_id=where, device_id_type=pl.DeviceIdType.MESH)

    load_q.wait()
    for l in range(layers):
        for k in range(QH):
            h, g = k // GROUP, k % GROUP
            q_f32[h, l * GROUP + g : l * GROUP + g + 1, :] = q_row[
                l : l + 1, k * HD : (k + 1) * HD
            ].astype(jnp.float32)
    q_send[...] = q_f32[...].astype(jnp.bfloat16)

    pl.semaphore_wait(barrier, n_all - 1)

    my_head = me_seq // span
    own_q = pltpu.make_async_copy(q_send.at[my_head], q_recv.at[me], q_recv_sem)
    own_q.start()

    @pl.loop(1, n_all)
    def _(k):
        other, where = place(k)
        pltpu.make_async_remote_copy(
            src_ref=q_send.at[other // n_rep // span],
            dst_ref=q_recv.at[me],
            send_sem=q_send_sem,
            recv_sem=q_recv_sem,
            device_id=where,
            device_id_type=pl.DeviceIdType.MESH,
        ).start()

    load_sfx.wait()
    s_rows = KVH * rows
    load_len.wait()
    load_slot.wait()
    length = lengths[slot[0]]
    q_all = q_f32[...].reshape(s_rows, HD)
    head_of = lax.broadcasted_iota(jnp.int32, (s_rows, HD), 0) // rows
    q_diag = jnp.concatenate(
        [jnp.where(head_of == h, q_all, 0.0) for h in range(KVH)], axis=1
    ).astype(jnp.bfloat16)
    suf = sfx.shape[3]
    lay_s = layer_rows((s_rows, suf), layers)
    scores = jnp.zeros((s_rows, suf), jnp.float32)
    for l in range(layers):
        part = lax.dot_general(q_diag, sfx[l, 0, 0], NT, preferred_element_type=jnp.float32)
        scores = jnp.where(lay_s == l, part, scores)
    valid = lax.broadcasted_iota(jnp.int32, (s_rows, suf), 1) < length
    scores = jnp.where(valid, scores * SCALE, neg_fill)
    s_top = jnp.max(scores, axis=1, keepdims=True)
    s_w = jnp.where(valid, jnp.exp2(scores - s_top), 0.0).astype(jnp.bfloat16)
    s_den = jnp.sum(s_w.astype(jnp.float32), axis=1, keepdims=True)
    lay_h = layer_rows((s_rows, HD), layers)
    s_num = jnp.zeros((s_rows, HD), jnp.float32)
    for l in range(layers):
        part = jnp.dot(s_w, sfx[l, 0, 1], preferred_element_type=jnp.float32)
        for h in range(KVH):
            s_num = jnp.where(
                (head_of == h) & (lay_h == l), part[:, h * HD : (h + 1) * HD], s_num
            )

    load_kv.wait()
    pltpu.make_async_copy(q_recv, q_recv, q_recv_sem).wait()

    chunk = min(CHUNK, n_all)
    c_rows = chunk * rows
    positions = kv.shape[3]

    def one_chunk(base):
        q_c = q_recv[pl.ds(base, chunk)].astype(jnp.float32).reshape(c_rows, HD)
        lay = layer_rows((c_rows, HD), layers)
        q_c = jnp.concatenate(
            [jnp.where(lay == l, q_c, 0.0) for l in range(layers)], axis=1
        ).astype(jnp.bfloat16)
        keys = kv[:, 0].reshape(layers * HD, positions)
        values = kv[:, 1].reshape(layers * HD, positions)
        s = jnp.dot(q_c, keys, preferred_element_type=jnp.float32) * SCALE
        top = jnp.max(s, axis=1, keepdims=True)
        w = jnp.exp2(s - top).astype(jnp.bfloat16)
        den = jnp.sum(w.astype(jnp.float32), axis=1, keepdims=True)
        num_all = lax.dot_general(w, values, NT, preferred_element_type=jnp.float32)
        num = num_all[:, :HD]
        for l in range(1, layers):
            num = jnp.where(lay == l, num_all[:, l * HD : (l + 1) * HD], num)
        lse = top + jnp.log2(den)
        high = lse.astype(jnp.bfloat16).astype(jnp.float32)
        mid = (lse - high).astype(jnp.bfloat16).astype(jnp.float32)
        low = lse - high - mid
        lane = lax.broadcasted_iota(jnp.int32, (c_rows, HD), 1)
        stat = jnp.where(lane == 0, high, jnp.where(lane == 1, mid, jnp.where(lane == 2, low, 0.0)))
        both = jnp.concatenate(
            [(num / den).reshape(chunk, rows, HD), stat.reshape(chunk, rows, HD)], axis=1
        )
        o_send[pl.ds(base, chunk)] = both.astype(jnp.bfloat16)

    if chunk == n_all:
        one_chunk(0)
    else:
        @pl.loop(0, n_all // chunk)
        def _(c):
            one_chunk(c * chunk)

    own_o = pltpu.make_async_copy(o_send.at[me], o_recv.at[me], o_recv_sem)
    own_o.start()

    @pl.loop(1, n_all)
    def _(k):
        other, where = place(k)
        pltpu.make_async_remote_copy(
            src_ref=o_send.at[other],
            dst_ref=o_recv.at[me],
            send_sem=o_send_sem,
            recv_sem=o_recv_sem,
            device_id=where,
            device_id_type=pl.DeviceIdType.MESH,
        ).start()

    s_out = (s_num / s_den).reshape(KVH, rows, HD)
    s_lse = (s_top + jnp.log2(s_den)).reshape(KVH, rows, 1)
    others = pl.ds(0, n_all - 1)
    sent_q = q_recv.at[others]
    pltpu.make_async_copy(sent_q, sent_q, q_send_sem).wait()
    pltpu.make_async_copy(o_recv, o_recv, o_recv_sem).wait()

    per_head = n_all // KVH
    for h in range(KVH):
        got = o_recv[h * per_head : (h + 1) * per_head].astype(jnp.float32)
        part = got[:, :rows]
        lse = jnp.sum(got[:, rows:], axis=2, keepdims=True)
        top = jnp.maximum(jnp.max(lse, axis=0), s_lse[h])
        wgt = jnp.exp2(lse - top[None])
        s_wgt = jnp.exp2(s_lse[h] - top)
        num = jnp.sum(wgt * part, axis=0) + s_wgt * s_out[h]
        den = jnp.sum(wgt, axis=0) + s_wgt
        mixed = num / den
        for l in range(layers):
            for g in range(GROUP):
                at = (h * GROUP + g) * HD
                r = l * GROUP + g
                out_ref[l : l + 1, at : at + HD] = mixed[r : r + 1].astype(out_ref.dtype)

    sent_o = o_recv.at[others]
    pltpu.make_async_copy(sent_o, sent_o, o_send_sem).wait()


def attend(n_seq, n_rep, prefix_cache, queries, suffix_cache, suffix_lengths, slot_request):
    layers, _, width = queries.shape
    n_all = n_seq * n_rep
    features = prefix_cache.shape[2]
    span = HD // features
    if span > 1:
        groups = [[h * span + j for j in range(span)] for h in range(n_seq // span)]
        prefix_cache = lax.all_to_all(
            prefix_cache, "seq", split_axis=3, concat_axis=2, axis_index_groups=groups, tiled=True
        )
    rows = layers * GROUP
    any_spec = pl.BlockSpec(memory_space=pltpu.HBM)
    queries = queries.reshape(layers, width)
    out = pl.pallas_call(
        functools.partial(kernel, n_rep, n_all, span, layers),
        out_shape=jax.ShapeDtypeStruct(queries.shape, queries.dtype),
        in_specs=[any_spec, any_spec, any_spec, any_spec, any_spec],
        out_specs=pl.BlockSpec(memory_space=pltpu.VMEM),
        scratch_shapes=[
            pltpu.VMEM(prefix_cache.shape, jnp.bfloat16),
            pltpu.VMEM(suffix_cache.shape, jnp.bfloat16),
            pltpu.VMEM(queries.shape, jnp.bfloat16),
            pltpu.VMEM((KVH, rows, HD), jnp.float32),
            pltpu.VMEM((KVH, rows, HD), jnp.bfloat16),
            pltpu.VMEM((n_all, rows, HD), jnp.bfloat16),
            pltpu.VMEM((n_all, 2 * rows, HD), jnp.bfloat16),
            pltpu.VMEM((n_all, 2 * rows, HD), jnp.bfloat16),
            pltpu.SMEM(suffix_lengths.shape, jnp.int32),
            pltpu.SMEM(slot_request.shape, jnp.int32),
            pltpu.SemaphoreType.DMA((5,)),
            pltpu.SemaphoreType.DMA,
            pltpu.SemaphoreType.DMA,
            pltpu.SemaphoreType.DMA,
            pltpu.SemaphoreType.DMA,
        ],
        compiler_params=pltpu.CompilerParams(collective_id=0, has_side_effects=True),
    )(suffix_lengths, slot_request, prefix_cache, queries, suffix_cache)
    return out.reshape(layers, 1, width)


def solution(mesh):
    in_specs = (
        P(None, None, "seq", "rep"),
        P(None, ("seq", "rep"), None),
        P(None, ("seq", "rep"), None, None, None),
        P(),
        P(("seq", "rep")),
    )
    return jax.shard_map(
        functools.partial(attend, mesh.shape["seq"], mesh.shape["rep"]),
        mesh=mesh,
        in_specs=in_specs,
        out_specs=P(None, ("seq", "rep"), None),
        check_vma=False,
    )
```

```python
import functools

import jax
import jax.numpy as jnp
from jax import lax
from jax.experimental import pallas as pl
from jax.experimental.pallas import tpu as pltpu
from jax.sharding import PartitionSpec as P

QH = 32
KVH = 8
HD = 128
GROUP = QH // KVH
neg_fill = -1e30
LOG2E = 1.4426950408889634
SCALE = HD ** -0.5 * LOG2E
CHUNK = 32
UNROLLED = 64
NT = (((1,), (1,)), ((), ()))


def layer_rows(shape, layers):
    return (lax.broadcasted_iota(jnp.int32, shape, 0) // GROUP) % layers


def hops(bits):
    return bits[1] + bin(bits[0] // 2).count("1")


def flip(x, bits, size):
    if size & (size - 1):
        return lax.rem(x + bits, size)
    step = 1
    while step < size:
        if bits & step:
            x = x + step - 2 * step * ((x // step) % 2)
        step *= 2
    return x


def kernel(
    n_rep, n_all, span, layers,
    lengths_ref, slot_ref, cache_ref, q_ref, suffix_ref, out_ref,
    kv, sfx, q_row, q_f32, q_send, q_recv, o_send, o_recv, lengths, slot,
    load_sem, q_send_sem, q_recv_sem, o_send_sem, o_recv_sem,
):
    rows = layers * GROUP
    me_seq = lax.axis_index("seq")
    me_rep = lax.axis_index("rep")
    me = me_seq * n_rep + me_rep

    n_seq = n_all // n_rep

    def each_partner(act):
        if n_all > UNROLLED:
            @pl.loop(1, n_all)
            def _(k):
                other = lax.rem(me + k, n_all)
                act(other, {"seq": other // n_rep, "rep": lax.rem(other, n_rep)})
        else:
            for bits_seq, bits_rep in sorted(((e, d) for d in range(n_rep) for e in range(n_seq)), key=hops, reverse=True):
                if bits_seq or bits_rep:
                    to_seq = flip(me_seq, bits_seq, n_seq)
                    to_rep = flip(me_rep, bits_rep, n_rep)
                    act(to_seq * n_rep + to_rep, {"seq": to_seq, "rep": to_rep})

    load_q = pltpu.make_async_copy(q_ref, q_row, load_sem.at[0])
    load_q.start()
    load_len = pltpu.make_async_copy(lengths_ref, lengths, load_sem.at[3])
    load_len.start()
    load_slot = pltpu.make_async_copy(slot_ref, slot, load_sem.at[4])
    load_slot.start()
    load_sfx = pltpu.make_async_copy(suffix_ref, sfx, load_sem.at[1])
    load_sfx.start()
    load_kv = pltpu.make_async_copy(cache_ref, kv, load_sem.at[2])
    load_kv.start()

    barrier = pltpu.get_barrier_semaphore()

    @each_partner
    def _(_, where):
        pl.semaphore_signal(barrier, inc=1, device_id=where, device_id_type=pl.DeviceIdType.MESH)

    load_q.wait()
    for l in range(layers):
        for k in range(QH):
            h, g = k // GROUP, k % GROUP
            q_f32[h, l * GROUP + g : l * GROUP + g + 1, :] = q_row[
                l : l + 1, k * HD : (k + 1) * HD
            ].astype(jnp.float32)
    q_send[...] = q_f32[...].astype(jnp.bfloat16)

    pl.semaphore_wait(barrier, n_all - 1)

    my_head = me_seq // span
    own_q = pltpu.make_async_copy(q_send.at[my_head], q_recv.at[me], q_recv_sem)
    own_q.start()

    @each_partner
    def _(other, where):
        pltpu.make_async_remote_copy(
            src_ref=q_send.at[other // n_rep // span],
            dst_ref=q_recv.at[me],
            send_sem=q_send_sem,
            recv_sem=q_recv_sem,
            device_id=where,
            device_id_type=pl.DeviceIdType.MESH,
        ).start()

    load_sfx.wait()
    s_rows = KVH * rows
    load_len.wait()
    load_slot.wait()
    length = lengths[slot[0]]
    q_all = q_f32[...].reshape(s_rows, HD)
    head_of = lax.broadcasted_iota(jnp.int32, (s_rows, HD), 0) // rows
    q_diag = jnp.concatenate(
        [jnp.where(head_of == h, q_all, 0.0) for h in range(KVH)], axis=1
    ).astype(jnp.bfloat16)
    suf = sfx.shape[3]
    lay_s = layer_rows((s_rows, suf), layers)
    scores = jnp.zeros((s_rows, suf), jnp.float32)
    for l in range(layers):
        part = lax.dot_general(q_diag, sfx[l, 0, 0], NT, preferred_element_type=jnp.float32)
        scores = jnp.where(lay_s == l, part, scores)
    valid = lax.broadcasted_iota(jnp.int32, (s_rows, suf), 1) < length
    scores = jnp.where(valid, scores * SCALE, neg_fill)
    s_top = jnp.max(scores, axis=1, keepdims=True)
    s_w = jnp.where(valid, jnp.exp2(scores - s_top), 0.0).astype(jnp.bfloat16)
    s_den = jnp.sum(s_w.astype(jnp.float32), axis=1, keepdims=True)
    lay_h = layer_rows((s_rows, HD), layers)
    s_num = jnp.zeros((s_rows, HD), jnp.float32)
    for l in range(layers):
        part = jnp.dot(s_w, sfx[l, 0, 1], preferred_element_type=jnp.float32)
        for h in range(KVH):
            s_num = jnp.where(
                (head_of == h) & (lay_h == l), part[:, h * HD : (h + 1) * HD], s_num
            )

    load_kv.wait()
    pltpu.make_async_copy(q_recv, q_recv, q_recv_sem).wait()

    chunk = min(CHUNK, n_all)
    c_rows = chunk * rows
    positions = kv.shape[3]

    def one_chunk(base):
        q_c = q_recv[pl.ds(base, chunk)].astype(jnp.float32).reshape(c_rows, HD)
        lay = layer_rows((c_rows, HD), layers)
        q_c = jnp.concatenate(
            [jnp.where(lay == l, q_c, 0.0) for l in range(layers)], axis=1
        ).astype(jnp.bfloat16)
        keys = kv[:, 0].reshape(layers * HD, positions)
        values = kv[:, 1].reshape(layers * HD, positions)
        s = jnp.dot(q_c, keys, preferred_element_type=jnp.float32) * SCALE
        top = jnp.max(s, axis=1, keepdims=True)
        w = jnp.exp2(s - top).astype(jnp.bfloat16)
        den = jnp.sum(w.astype(jnp.float32), axis=1, keepdims=True)
        num_all = lax.dot_general(w, values, NT, preferred_element_type=jnp.float32)
        num = num_all[:, :HD]
        for l in range(1, layers):
            num = jnp.where(lay == l, num_all[:, l * HD : (l + 1) * HD], num)
        lse = top + jnp.log2(den)
        high = lse.astype(jnp.bfloat16).astype(jnp.float32)
        mid = (lse - high).astype(jnp.bfloat16).astype(jnp.float32)
        low = lse - high - mid
        lane = lax.broadcasted_iota(jnp.int32, (c_rows, HD), 1)
        stat = jnp.where(lane == 0, high, jnp.where(lane == 1, mid, jnp.where(lane == 2, low, 0.0)))
        both = jnp.concatenate(
            [(num / den).reshape(chunk, rows, HD), stat.reshape(chunk, rows, HD)], axis=1
        )
        o_send[pl.ds(base, chunk)] = both.astype(jnp.bfloat16)

    if chunk == n_all:
        one_chunk(0)
    else:
        @pl.loop(0, n_all // chunk)
        def _(c):
            one_chunk(c * chunk)

    own_o = pltpu.make_async_copy(o_send.at[me], o_recv.at[me], o_recv_sem)
    own_o.start()

    @each_partner
    def _(other, where):
        pltpu.make_async_remote_copy(
            src_ref=o_send.at[other],
            dst_ref=o_recv.at[me],
            send_sem=o_send_sem,
            recv_sem=o_recv_sem,
            device_id=where,
            device_id_type=pl.DeviceIdType.MESH,
        ).start()

    s_out = (s_num / s_den).reshape(KVH, rows, HD)
    s_lse = (s_top + jnp.log2(s_den)).reshape(KVH, rows, 1)
    others = pl.ds(0, n_all - 1)
    sent_q = q_recv.at[others]
    pltpu.make_async_copy(sent_q, sent_q, q_send_sem).wait()
    pltpu.make_async_copy(o_recv, o_recv, o_recv_sem).wait()

    per_head = n_all // KVH
    for h in range(KVH):
        got = o_recv[h * per_head : (h + 1) * per_head].astype(jnp.float32)
        part = got[:, :rows]
        lse = jnp.sum(got[:, rows:], axis=2, keepdims=True)
        top = jnp.maximum(jnp.max(lse, axis=0), s_lse[h])
        wgt = jnp.exp2(lse - top[None])
        s_wgt = jnp.exp2(s_lse[h] - top)
        num = jnp.sum(wgt * part, axis=0) + s_wgt * s_out[h]
        den = jnp.sum(wgt, axis=0) + s_wgt
        mixed = num / den
        for l in range(layers):
            for g in range(GROUP):
                at = (h * GROUP + g) * HD
                r = l * GROUP + g
                out_ref[l : l + 1, at : at + HD] = mixed[r : r + 1].astype(out_ref.dtype)

    sent_o = o_recv.at[others]
    pltpu.make_async_copy(sent_o, sent_o, o_send_sem).wait()


def attend(n_seq, n_rep, prefix_cache, queries, suffix_cache, suffix_lengths, slot_request):
    layers, _, width = queries.shape
    n_all = n_seq * n_rep
    features = prefix_cache.shape[2]
    span = HD // features
    if span > 1:
        groups = [[h * span + j for j in range(span)] for h in range(n_seq // span)]
        prefix_cache = lax.all_to_all(
            prefix_cache, "seq", split_axis=3, concat_axis=2, axis_index_groups=groups, tiled=True
        )
    rows = layers * GROUP
    any_spec = pl.BlockSpec(memory_space=pltpu.HBM)
    queries = queries.reshape(layers, width)
    out = pl.pallas_call(
        functools.partial(kernel, n_rep, n_all, span, layers),
        out_shape=pltpu.VMEM(queries.shape, queries.dtype),
        in_specs=[any_spec, any_spec, any_spec, any_spec, any_spec],
        out_specs=pl.BlockSpec(memory_space=pltpu.VMEM),
        scratch_shapes=[
            pltpu.VMEM(prefix_cache.shape, jnp.bfloat16),
            pltpu.VMEM(suffix_cache.shape, jnp.bfloat16),
            pltpu.VMEM(queries.shape, jnp.bfloat16),
            pltpu.VMEM((KVH, rows, HD), jnp.float32),
            pltpu.VMEM((KVH, rows, HD), jnp.bfloat16),
            pltpu.VMEM((n_all, rows, HD), jnp.bfloat16),
            pltpu.VMEM((n_all, 2 * rows, HD), jnp.bfloat16),
            pltpu.VMEM((n_all, 2 * rows, HD), jnp.bfloat16),
            pltpu.SMEM(suffix_lengths.shape, jnp.int32),
            pltpu.SMEM(slot_request.shape, jnp.int32),
            pltpu.SemaphoreType.DMA((5,)),
            pltpu.SemaphoreType.DMA,
            pltpu.SemaphoreType.DMA,
            pltpu.SemaphoreType.DMA,
            pltpu.SemaphoreType.DMA,
        ],
        compiler_params=pltpu.CompilerParams(collective_id=0, has_side_effects=True),
    )(suffix_lengths, slot_request, prefix_cache, queries, suffix_cache)
    return out.reshape(layers, 1, width)


def solution(mesh):
    in_specs = (
        P(None, None, "seq", "rep"),
        P(None, ("seq", "rep"), None),
        P(None, ("seq", "rep"), None, None, None),
        P(),
        P(("seq", "rep")),
    )
    return jax.shard_map(
        functools.partial(attend, mesh.shape["seq"], mesh.shape["rep"]),
        mesh=mesh,
        in_specs=in_specs,
        out_specs=P(None, ("seq", "rep"), None),
        check_vma=False,
    )
```

```python
import functools

import jax
import jax.numpy as jnp
from jax import lax
from jax.experimental import pallas as pl
from jax.experimental.pallas import tpu as pltpu
from jax.sharding import PartitionSpec as P

QH = 32
KVH = 8
HD = 128
GROUP = QH // KVH
neg_fill = -1e30
LOG2E = 1.4426950408889634
SCALE = HD ** -0.5 * LOG2E
CHUNK = 32
UNROLLED = 8
NT = (((1,), (1,)), ((), ()))


def layer_rows(shape, layers):
    return (lax.broadcasted_iota(jnp.int32, shape, 0) // GROUP) % layers


def flip(x, bits):
    step = 1
    while step <= bits:
        if bits & step:
            x = x + step - 2 * step * ((x // step) % 2)
        step *= 2
    return x


def hops(bits):
    return bits[1] + bin(bits[0] // 2).count("1")


def kernel(
    n_rep, n_all, span, layers,
    lengths_ref, slot_ref, cache_ref, q_ref, suffix_ref, out_ref,
    kv, sfx, q_row, q_f32, q_send, q_recv, o_send, o_recv, lengths, slot,
    load_sem, q_send_sem, q_recv_sem, o_send_sem, o_recv_sem,
):
    rows = layers * GROUP
    me_seq = lax.axis_index("seq")
    me_rep = lax.axis_index("rep")

    n_seq = n_all // n_rep

    def each_partner(distances):
        def run(act):
            if n_seq > UNROLLED:
                for d in distances:
                    to_rep = flip(me_rep, d)

                    @pl.loop(0 if d else 1, n_seq)
                    def _(e):
                        act(lax.rem(me_seq + e, n_seq), to_rep, d)
            else:
                pairs = [(e, d) for d in distances for e in range(n_seq) if e or d]
                for e, d in sorted(pairs, key=hops, reverse=True):
                    act(flip(me_seq, e), flip(me_rep, d), d)

        return run

    load_q = pltpu.make_async_copy(q_ref, q_row, load_sem.at[0])
    load_q.start()
    load_len = pltpu.make_async_copy(lengths_ref, lengths, load_sem.at[3])
    load_len.start()
    load_slot = pltpu.make_async_copy(slot_ref, slot, load_sem.at[4])
    load_slot.start()
    load_sfx = pltpu.make_async_copy(suffix_ref, sfx, load_sem.at[1])
    load_sfx.start()
    load_kv = pltpu.make_async_copy(cache_ref, kv, load_sem.at[2])
    load_kv.start()

    barrier = pltpu.get_barrier_semaphore()

    @each_partner(range(n_rep))
    def _(to_seq, to_rep, d):
        where = {"seq": to_seq, "rep": to_rep}
        pl.semaphore_signal(barrier, inc=1, device_id=where, device_id_type=pl.DeviceIdType.MESH)

    load_q.wait()
    for l in range(layers):
        for k in range(QH):
            h, g = k // GROUP, k % GROUP
            q_f32[h, l * GROUP + g : l * GROUP + g + 1, :] = q_row[
                l : l + 1, k * HD : (k + 1) * HD
            ].astype(jnp.float32)
    q_send[...] = q_f32[...].astype(jnp.bfloat16)

    pl.semaphore_wait(barrier, n_all - 1)

    my_head = me_seq // span
    splits = [[d] for d in range(n_rep)]
    group_of = {d: i for i, group in enumerate(splits) for d in group}
    own_q = pltpu.make_async_copy(
        q_send.at[my_head], q_recv.at[0, me_seq], q_recv_sem.at[group_of[0]]
    )
    own_q.start()

    @each_partner(range(n_rep))
    def _(to_seq, to_rep, d):
        pltpu.make_async_remote_copy(
            src_ref=q_send.at[to_seq // span],
            dst_ref=q_recv.at[d, me_seq],
            send_sem=q_send_sem,
            recv_sem=q_recv_sem.at[group_of[d]],
            device_id={"seq": to_seq, "rep": to_rep},
            device_id_type=pl.DeviceIdType.MESH,
        ).start()

    load_sfx.wait()
    s_rows = KVH * rows
    load_len.wait()
    load_slot.wait()
    length = lengths[slot[0]]
    q_all = q_f32[...].reshape(s_rows, HD)
    head_of = lax.broadcasted_iota(jnp.int32, (s_rows, HD), 0) // rows
    q_diag = jnp.concatenate(
        [jnp.where(head_of == h, q_all, 0.0) for h in range(KVH)], axis=1
    ).astype(jnp.bfloat16)
    suf = sfx.shape[3]
    lay_s = layer_rows((s_rows, suf), layers)
    scores = jnp.zeros((s_rows, suf), jnp.float32)
    for l in range(layers):
        part = lax.dot_general(q_diag, sfx[l, 0, 0], NT, preferred_element_type=jnp.float32)
        scores = jnp.where(lay_s == l, part, scores)
    valid = lax.broadcasted_iota(jnp.int32, (s_rows, suf), 1) < length
    scores = jnp.where(valid, scores * SCALE, neg_fill)
    s_top = jnp.max(scores, axis=1, keepdims=True)
    s_w = jnp.where(valid, jnp.exp2(scores - s_top), 0.0).astype(jnp.bfloat16)
    s_den = jnp.sum(s_w.astype(jnp.float32), axis=1, keepdims=True)
    lay_h = layer_rows((s_rows, HD), layers)
    s_num = jnp.zeros((s_rows, HD), jnp.float32)
    for l in range(layers):
        part = jnp.dot(s_w, sfx[l, 0, 1], preferred_element_type=jnp.float32)
        for h in range(KVH):
            s_num = jnp.where(
                (head_of == h) & (lay_h == l), part[:, h * HD : (h + 1) * HD], s_num
            )

    load_kv.wait()

    positions = kv.shape[3]

    def one_chunk(d, base, reps, chunk):
        c_rows = reps * chunk * rows
        here = (pl.ds(d, reps), pl.ds(base, chunk))
        q_c = q_recv[here].astype(jnp.float32).reshape(c_rows, HD)
        lay = layer_rows((c_rows, HD), layers)
        q_c = jnp.concatenate(
            [jnp.where(lay == l, q_c, 0.0) for l in range(layers)], axis=1
        ).astype(jnp.bfloat16)
        keys = kv[:, 0].reshape(layers * HD, positions)
        values = kv[:, 1].reshape(layers * HD, positions)
        s = jnp.dot(q_c, keys, preferred_element_type=jnp.float32) * SCALE
        top = jnp.max(s, axis=1, keepdims=True)
        w = jnp.exp2(s - top).astype(jnp.bfloat16)
        den = jnp.sum(w.astype(jnp.float32), axis=1, keepdims=True)
        num_all = lax.dot_general(w, values, NT, preferred_element_type=jnp.float32)
        num = num_all[:, :HD]
        for l in range(1, layers):
            num = jnp.where(lay == l, num_all[:, l * HD : (l + 1) * HD], num)
        lse = top + jnp.log2(den)
        high = lse.astype(jnp.bfloat16).astype(jnp.float32)
        mid = (lse - high).astype(jnp.bfloat16).astype(jnp.float32)
        low = lse - high - mid
        lane = lax.broadcasted_iota(jnp.int32, (c_rows, HD), 1)
        stat = jnp.where(lane == 0, high, jnp.where(lane == 1, mid, jnp.where(lane == 2, low, 0.0)))
        both = jnp.concatenate(
            [(num / den).reshape(reps, chunk, rows, HD), stat.reshape(reps, chunk, rows, HD)], axis=2
        )
        o_send[here] = both.astype(jnp.bfloat16)

    for i, group in enumerate(splits):
        landed = q_recv.at[pl.ds(group[0], len(group))]
        pltpu.make_async_copy(landed, landed, q_recv_sem.at[i]).wait()
        if n_seq * len(group) <= CHUNK:
            one_chunk(group[0], 0, len(group), n_seq)
        else:
            for d in group:
                chunk = min(CHUNK, n_seq)

                @pl.loop(0, n_seq // chunk)
                def _(c, d=d, chunk=chunk):
                    one_chunk(d, c * chunk, 1, chunk)

        if 0 in group:
            own_o = pltpu.make_async_copy(o_send.at[0, me_seq], o_recv.at[0, me_seq], o_recv_sem)
            own_o.start()

        @each_partner(group)
        def _(to_seq, to_rep, d):
            pltpu.make_async_remote_copy(
                src_ref=o_send.at[d, to_seq],
                dst_ref=o_recv.at[d, me_seq],
                send_sem=o_send_sem,
                recv_sem=o_recv_sem,
                device_id={"seq": to_seq, "rep": to_rep},
                device_id_type=pl.DeviceIdType.MESH,
            ).start()

    s_out = (s_num / s_den).reshape(KVH, rows, HD)
    s_lse = (s_top + jnp.log2(s_den)).reshape(KVH, rows, 1)
    pltpu.make_async_copy(o_recv, o_recv, o_recv_sem).wait()

    per_head = n_seq // KVH
    for h in range(KVH):
        got = o_recv[:, h * per_head : (h + 1) * per_head].astype(jnp.float32)
        got = got.reshape(n_rep * per_head, 2 * rows, HD)
        part = got[:, :rows]
        lse = jnp.sum(got[:, rows:], axis=2, keepdims=True)
        top = jnp.maximum(jnp.max(lse, axis=0), s_lse[h])
        wgt = jnp.exp2(lse - top[None])
        s_wgt = jnp.exp2(s_lse[h] - top)
        num = jnp.sum(wgt * part, axis=0) + s_wgt * s_out[h]
        den = jnp.sum(wgt, axis=0) + s_wgt
        mixed = num / den
        for l in range(layers):
            for g in range(GROUP):
                at = (h * GROUP + g) * HD
                r = l * GROUP + g
                out_ref[l : l + 1, at : at + HD] = mixed[r : r + 1].astype(out_ref.dtype)

    sent_q = (q_recv.at[pl.ds(0, n_rep - 1)], q_recv.at[n_rep - 1, pl.ds(0, n_seq - 1)])
    for sent in sent_q:
        pltpu.make_async_copy(sent, sent, q_send_sem).wait()
    sent_o = (o_recv.at[pl.ds(0, n_rep - 1)], o_recv.at[n_rep - 1, pl.ds(0, n_seq - 1)])
    for sent in sent_o:
        pltpu.make_async_copy(sent, sent, o_send_sem).wait()


def attend(n_seq, n_rep, prefix_cache, queries, suffix_cache, suffix_lengths, slot_request):
    layers, _, width = queries.shape
    n_all = n_seq * n_rep
    features = prefix_cache.shape[2]
    span = HD // features
    if span > 1:
        groups = [[h * span + j for j in range(span)] for h in range(n_seq // span)]
        prefix_cache = lax.all_to_all(
            prefix_cache, "seq", split_axis=3, concat_axis=2, axis_index_groups=groups, tiled=True
        )
    rows = layers * GROUP
    any_spec = pl.BlockSpec(memory_space=pltpu.HBM)
    queries = queries.reshape(layers, width)
    out = pl.pallas_call(
        functools.partial(kernel, n_rep, n_all, span, layers),
        out_shape=pltpu.VMEM(queries.shape, queries.dtype),
        in_specs=[any_spec, any_spec, any_spec, any_spec, any_spec],
        out_specs=pl.BlockSpec(memory_space=pltpu.VMEM),
        scratch_shapes=[
            pltpu.VMEM(prefix_cache.shape, jnp.bfloat16),
            pltpu.VMEM(suffix_cache.shape, jnp.bfloat16),
            pltpu.VMEM(queries.shape, jnp.bfloat16),
            pltpu.VMEM((KVH, rows, HD), jnp.float32),
            pltpu.VMEM((KVH, rows, HD), jnp.bfloat16),
            pltpu.VMEM((n_rep, n_seq, rows, HD), jnp.bfloat16),
            pltpu.VMEM((n_rep, n_seq, 2 * rows, HD), jnp.bfloat16),
            pltpu.VMEM((n_rep, n_seq, 2 * rows, HD), jnp.bfloat16),
            pltpu.SMEM(suffix_lengths.shape, jnp.int32),
            pltpu.SMEM(slot_request.shape, jnp.int32),
            pltpu.SemaphoreType.DMA((5,)),
            pltpu.SemaphoreType.DMA,
            pltpu.SemaphoreType.DMA((n_rep,)),
            pltpu.SemaphoreType.DMA,
            pltpu.SemaphoreType.DMA,
        ],
        compiler_params=pltpu.CompilerParams(collective_id=0, has_side_effects=True),
    )(suffix_lengths, slot_request, prefix_cache, queries, suffix_cache)
    return out.reshape(layers, 1, width)


def solution(mesh):
    in_specs = (
        P(None, None, "seq", "rep"),
        P(None, ("seq", "rep"), None),
        P(None, ("seq", "rep"), None, None, None),
        P(),
        P(("seq", "rep")),
    )
    return jax.shard_map(
        functools.partial(attend, mesh.shape["seq"], mesh.shape["rep"]),
        mesh=mesh,
        in_specs=in_specs,
        out_specs=P(None, ("seq", "rep"), None),
        check_vma=False,
    )
```

```python
import functools

import jax
import jax.numpy as jnp
from jax import lax
from jax.experimental import pallas as pl
from jax.experimental.pallas import tpu as pltpu
from jax.sharding import PartitionSpec as P

QH = 32
KVH = 8
HD = 128
GROUP = QH // KVH
neg_fill = -1e30
LOG2E = 1.4426950408889634
SCALE = HD ** -0.5 * LOG2E
CHUNK = 32
UNROLLED = 8
NT = (((1,), (1,)), ((), ()))


def layer_rows(shape, layers):
    return (lax.broadcasted_iota(jnp.int32, shape, 0) // GROUP) % layers


def flip(x, bits):
    step = 1
    while step <= bits:
        if bits & step:
            x = x + step - 2 * step * ((x // step) % 2)
        step *= 2
    return x


def hops(bits):
    return bits[1] + bin(bits[0] // 2).count("1")


def kernel(
    n_rep, n_all, span, layers,
    lengths_ref, slot_ref, cache_ref, q_ref, suffix_ref, out_ref,
    kv, vt, sfx, q_row, q_f32, q_send, q_recv, o_send, o_recv, lengths, slot,
    load_sem, q_send_sem, q_recv_sem, o_send_sem, o_recv_sem,
):
    rows = layers * GROUP
    me_seq = lax.axis_index("seq")
    me_rep = lax.axis_index("rep")

    n_seq = n_all // n_rep

    def each_partner(distances):
        def run(act):
            if n_seq > UNROLLED:
                for d in distances:
                    to_rep = flip(me_rep, d)

                    @pl.loop(0 if d else 1, n_seq)
                    def _(e):
                        act(lax.rem(me_seq + e, n_seq), to_rep, d)
            else:
                pairs = [(e, d) for d in distances for e in range(n_seq) if e or d]
                for e, d in sorted(pairs, key=hops, reverse=True):
                    act(flip(me_seq, e), flip(me_rep, d), d)

        return run

    barrier = pltpu.get_barrier_semaphore()

    @each_partner(range(n_rep))
    def _(to_seq, to_rep, d):
        where = {"seq": to_seq, "rep": to_rep}
        pl.semaphore_signal(barrier, inc=1, device_id=where, device_id_type=pl.DeviceIdType.MESH)

    load_q = pltpu.make_async_copy(q_ref, q_row, load_sem.at[0])
    load_q.start()
    load_len = pltpu.make_async_copy(lengths_ref, lengths, load_sem.at[3])
    load_len.start()
    load_slot = pltpu.make_async_copy(slot_ref, slot, load_sem.at[4])
    load_slot.start()
    load_sfx = pltpu.make_async_copy(suffix_ref, sfx, load_sem.at[1])
    load_sfx.start()
    load_kv = pltpu.make_async_copy(cache_ref, kv, load_sem.at[2])
    load_kv.start()

    load_q.wait()
    for l in range(layers):
        for k in range(QH):
            h, g = k // GROUP, k % GROUP
            q_f32[h, l * GROUP + g : l * GROUP + g + 1, :] = q_row[
                l : l + 1, k * HD : (k + 1) * HD
            ].astype(jnp.float32)
    q_send[...] = q_f32[...].astype(jnp.bfloat16)

    pl.semaphore_wait(barrier, n_all - 1)

    my_head = me_seq // span
    splits = [[d] for d in range(n_rep)]
    group_of = {d: i for i, group in enumerate(splits) for d in group}
    own_q = pltpu.make_async_copy(
        q_send.at[my_head], q_recv.at[0, me_seq], q_recv_sem.at[group_of[0]]
    )
    own_q.start()

    @each_partner(range(n_rep))
    def _(to_seq, to_rep, d):
        pltpu.make_async_remote_copy(
            src_ref=q_send.at[to_seq // span],
            dst_ref=q_recv.at[d, me_seq],
            send_sem=q_send_sem,
            recv_sem=q_recv_sem.at[group_of[d]],
            device_id={"seq": to_seq, "rep": to_rep},
            device_id_type=pl.DeviceIdType.MESH,
        ).start()

    load_sfx.wait()
    s_rows = KVH * rows
    load_len.wait()
    load_slot.wait()
    length = lengths[slot[0]]
    q_all = q_f32[...].reshape(s_rows, HD)
    head_of = lax.broadcasted_iota(jnp.int32, (s_rows, HD), 0) // rows
    q_diag = jnp.concatenate(
        [jnp.where(head_of == h, q_all, 0.0) for h in range(KVH)], axis=1
    ).astype(jnp.bfloat16)
    suf = sfx.shape[3]
    lay_s = layer_rows((s_rows, suf), layers)
    scores = jnp.zeros((s_rows, suf), jnp.float32)
    for l in range(layers):
        part = lax.dot_general(q_diag, sfx[l, 0, 0], NT, preferred_element_type=jnp.float32)
        scores = jnp.where(lay_s == l, part, scores)
    valid = lax.broadcasted_iota(jnp.int32, (s_rows, suf), 1) < length
    scores = jnp.where(valid, scores * SCALE, neg_fill)
    s_top = jnp.max(scores, axis=1, keepdims=True)
    s_w = jnp.where(valid, jnp.exp2(scores - s_top), 0.0).astype(jnp.bfloat16)
    s_den = jnp.sum(s_w.astype(jnp.float32), axis=1, keepdims=True)
    lay_h = layer_rows((s_rows, HD), layers)
    s_num = jnp.zeros((s_rows, HD), jnp.float32)
    for l in range(layers):
        part = jnp.dot(s_w, sfx[l, 0, 1], preferred_element_type=jnp.float32)
        for h in range(KVH):
            s_num = jnp.where(
                (head_of == h) & (lay_h == l), part[:, h * HD : (h + 1) * HD], s_num
            )

    load_kv.wait()

    positions = kv.shape[3]
    for l in range(layers):
        vt[:, l * HD : (l + 1) * HD] = kv[l, 1].T

    def one_chunk(d, base, reps, chunk):
        c_rows = reps * chunk * rows
        here = (pl.ds(d, reps), pl.ds(base, chunk))
        q_c = q_recv[here].astype(jnp.float32).reshape(c_rows, HD)
        lay = layer_rows((c_rows, HD), layers)
        q_c = jnp.concatenate(
            [jnp.where(lay == l, q_c, 0.0) for l in range(layers)], axis=1
        ).astype(jnp.bfloat16)
        keys = kv[:, 0].reshape(layers * HD, positions)
        s = jnp.dot(q_c, keys, preferred_element_type=jnp.float32) * SCALE
        top = jnp.max(s, axis=1, keepdims=True)
        w = jnp.exp2(s - top).astype(jnp.bfloat16)
        den = jnp.sum(w.astype(jnp.float32), axis=1, keepdims=True)
        num_all = jnp.dot(w, vt[...], preferred_element_type=jnp.float32)
        num = num_all[:, :HD]
        for l in range(1, layers):
            num = jnp.where(lay == l, num_all[:, l * HD : (l + 1) * HD], num)
        lse = top + jnp.log2(den)
        high = lse.astype(jnp.bfloat16).astype(jnp.float32)
        mid = (lse - high).astype(jnp.bfloat16).astype(jnp.float32)
        low = lse - high - mid
        lane = lax.broadcasted_iota(jnp.int32, (c_rows, HD), 1)
        stat = jnp.where(lane == 0, high, jnp.where(lane == 1, mid, jnp.where(lane == 2, low, 0.0)))
        both = jnp.concatenate(
            [(num / den).reshape(reps, chunk, rows, HD), stat.reshape(reps, chunk, rows, HD)], axis=2
        )
        o_send[here] = both.astype(jnp.bfloat16)

    for i, group in enumerate(splits):
        landed = q_recv.at[pl.ds(group[0], len(group))]
        pltpu.make_async_copy(landed, landed, q_recv_sem.at[i]).wait()
        if n_seq * len(group) <= CHUNK:
            one_chunk(group[0], 0, len(group), n_seq)
        else:
            for d in group:
                chunk = min(CHUNK, n_seq)

                @pl.loop(0, n_seq // chunk)
                def _(c, d=d, chunk=chunk):
                    one_chunk(d, c * chunk, 1, chunk)

        if 0 in group:
            own_o = pltpu.make_async_copy(o_send.at[0, me_seq], o_recv.at[0, me_seq], o_recv_sem)
            own_o.start()

        @each_partner(group)
        def _(to_seq, to_rep, d):
            pltpu.make_async_remote_copy(
                src_ref=o_send.at[d, to_seq],
                dst_ref=o_recv.at[d, me_seq],
                send_sem=o_send_sem,
                recv_sem=o_recv_sem,
                device_id={"seq": to_seq, "rep": to_rep},
                device_id_type=pl.DeviceIdType.MESH,
            ).start()

    s_out = (s_num / s_den).reshape(KVH, rows, HD)
    s_lse = (s_top + jnp.log2(s_den)).reshape(KVH, rows, 1)
    pltpu.make_async_copy(o_recv, o_recv, o_recv_sem).wait()

    per_head = n_seq // KVH
    for h in range(KVH):
        got = o_recv[:, h * per_head : (h + 1) * per_head].astype(jnp.float32)
        got = got.reshape(n_rep * per_head, 2 * rows, HD)
        part = got[:, :rows]
        lse = jnp.sum(got[:, rows:], axis=2, keepdims=True)
        top = jnp.maximum(jnp.max(lse, axis=0), s_lse[h])
        wgt = jnp.exp2(lse - top[None])
        s_wgt = jnp.exp2(s_lse[h] - top)
        num = jnp.sum(wgt * part, axis=0) + s_wgt * s_out[h]
        den = jnp.sum(wgt, axis=0) + s_wgt
        mixed = num / den
        for l in range(layers):
            for g in range(GROUP):
                at = (h * GROUP + g) * HD
                r = l * GROUP + g
                out_ref[l : l + 1, at : at + HD] = mixed[r : r + 1].astype(out_ref.dtype)

    sent_q = (q_recv.at[pl.ds(0, n_rep - 1)], q_recv.at[n_rep - 1, pl.ds(0, n_seq - 1)])
    for sent in sent_q:
        pltpu.make_async_copy(sent, sent, q_send_sem).wait()
    sent_o = (o_recv.at[pl.ds(0, n_rep - 1)], o_recv.at[n_rep - 1, pl.ds(0, n_seq - 1)])
    for sent in sent_o:
        pltpu.make_async_copy(sent, sent, o_send_sem).wait()


def attend(n_seq, n_rep, prefix_cache, queries, suffix_cache, suffix_lengths, slot_request):
    layers, _, width = queries.shape
    n_all = n_seq * n_rep
    features = prefix_cache.shape[2]
    span = HD // features
    if span > 1:
        groups = [[h * span + j for j in range(span)] for h in range(n_seq // span)]
        prefix_cache = lax.all_to_all(
            prefix_cache, "seq", split_axis=3, concat_axis=2, axis_index_groups=groups, tiled=True
        )
    rows = layers * GROUP
    any_spec = pl.BlockSpec(memory_space=pltpu.HBM)
    queries = queries.reshape(layers, width)
    out = pl.pallas_call(
        functools.partial(kernel, n_rep, n_all, span, layers),
        out_shape=pltpu.VMEM(queries.shape, queries.dtype),
        in_specs=[any_spec, any_spec, any_spec, any_spec, any_spec],
        out_specs=pl.BlockSpec(memory_space=pltpu.VMEM),
        scratch_shapes=[
            pltpu.VMEM(prefix_cache.shape, jnp.bfloat16),
            pltpu.VMEM((prefix_cache.shape[3], layers * HD), jnp.bfloat16),
            pltpu.VMEM(suffix_cache.shape, jnp.bfloat16),
            pltpu.VMEM(queries.shape, jnp.bfloat16),
            pltpu.VMEM((KVH, rows, HD), jnp.float32),
            pltpu.VMEM((KVH, rows, HD), jnp.bfloat16),
            pltpu.VMEM((n_rep, n_seq, rows, HD), jnp.bfloat16),
            pltpu.VMEM((n_rep, n_seq, 2 * rows, HD), jnp.bfloat16),
            pltpu.VMEM((n_rep, n_seq, 2 * rows, HD), jnp.bfloat16),
            pltpu.SMEM(suffix_lengths.shape, jnp.int32),
            pltpu.SMEM(slot_request.shape, jnp.int32),
            pltpu.SemaphoreType.DMA((5,)),
            pltpu.SemaphoreType.DMA,
            pltpu.SemaphoreType.DMA((n_rep,)),
            pltpu.SemaphoreType.DMA,
            pltpu.SemaphoreType.DMA,
        ],
        compiler_params=pltpu.CompilerParams(collective_id=0, has_side_effects=True),
    )(suffix_lengths, slot_request, prefix_cache, queries, suffix_cache)
    return out.reshape(layers, 1, width)


def solution(mesh):
    in_specs = (
        P(None, None, "seq", "rep"),
        P(None, ("seq", "rep"), None),
        P(None, ("seq", "rep"), None, None, None),
        P(),
        P(("seq", "rep")),
    )
    return jax.shard_map(
        functools.partial(attend, mesh.shape["seq"], mesh.shape["rep"]),
        mesh=mesh,
        in_specs=in_specs,
        out_specs=P(None, ("seq", "rep"), None),
        check_vma=False,
    )
```
